32 devices in a mesh: chol: 16 (over z, x, core), virt: 2 (over y).
Axes of the slice: x: 2, y: 2, z: 4, core: 2. Of those that a mesh axis runs over, the one named last changes fastest.
Arguments:
- amplitudes: bfloat16 [9600, 600], P('chol'), may hold values from -6 to 6
- chol_vectors: bfloat16 [128, 600, 600], P('chol', 'virt'), may hold values from -0.072753906 to 0.072753906
Outputs:
- sigma: float32 [9600, 600], P('chol', 'virt')
The draws below stay inside these ranges and needn't reach their ends.
All inputs are finite; a program needn't handle non-finite values.
Results may differ from the reference program's by a relative error of at most 0.0042.
Values may be sent and summed in bfloat16 or wider, within the bound.
A program may use at most 192 MiB of HBM per device.

```python
import jax
import jax.numpy as jnp
from jax import lax

V = 600
ROOTS = 2
PAIRS = 8
CH_DEV = 8
NP = 128
N_CHOL = 16


def levels(rng, dims, split, least, high):
    def one(axis_at, parts):
        steps = jax.random.uniform(jax.random.fold_in(jax.random.fold_in(rng, 6), axis_at), (parts,), jnp.float32, least / len(split), high / len(split))
        return jnp.repeat(jnp.exp(steps), dims[axis_at] // parts).reshape((-1,) + (1,) * (len(dims) - axis_at - 1))

    gain = one(*split[0])
    for cut in split[1:]:
        gain = gain * one(*cut)
    return gain


def scatter_about(key, shape, deviation, reach, shards=(), dtype=jnp.bfloat16):
    values = deviation * jax.random.normal(key, shape, jnp.float32)
    if shards:
        values = values * levels(key, shape, shards, -0.22, 0.18)
    return jnp.clip(values, -reach, reach).astype(dtype)


def setup_inputs(seed: int = 0) -> dict:
    streams_of = jax.random.split(jax.random.key(seed), 3)
    return {
        "amplitudes": scatter_about(streams_of[0], (ROOTS * PAIRS * V, V), 1.0, 6.0, ((0, 16),)),
        "chol_vectors": scatter_about(streams_of[1], (NP, V, V), ((V * (CH_DEV * N_CHOL) ** 0.5) ** -0.5), 0.072753906, ((0, 16), (1, 2))),
    }


def reference(amplitudes, chol_vectors):
    combos = ROOTS * PAIRS

    def one_vector(running, vector):
        ladder_half = jnp.dot(amplitudes, vector.T, preferred_element_type=jnp.float32).astype(jnp.bfloat16)
        ladder_half = ladder_half.reshape(combos, V, V)
        update = jnp.einsum('ac,ncb->nab', vector.astype(jnp.float32), ladder_half.astype(jnp.float32), precision=lax.Precision.HIGHEST)
        return running + update, None

    zeros_init = jnp.zeros((combos, V, V), jnp.float32)
    total, unused = lax.scan(one_vector, zeros_init, chol_vectors)
    return total.reshape(combos * V, V)
```

```python
import functools

import jax
import jax.numpy as jnp
from jax import lax
from jax.experimental import pallas as pl
from jax.experimental.pallas import tpu as pltpu
from jax.sharding import PartitionSpec as P

MESH = pl.DeviceIdType.MESH
KEPT = 4


def up(size, unit):
    return -(-size // unit) * unit


def plain(amplitudes, chol_vectors):
    vec_count, row_share, orbitals = chol_vectors.shape
    turned = jnp.transpose(chol_vectors, (1, 2, 0)).reshape(row_share, orbitals * vec_count)
    local_flat = chol_vectors.reshape(vec_count * row_share, orbitals)
    ladder_half = jnp.dot(
        lax.all_gather(amplitudes, "chol", axis=0, tiled=True),
        local_flat.T,
        preferred_element_type=jnp.float32,
    ).astype(jnp.bfloat16)
    combos = ladder_half.shape[0] // orbitals
    half_blocks = ladder_half.reshape(combos, orbitals * vec_count, row_share)
    sigma_terms = jnp.einsum(
        "ak,nkb->nab",
        lax.all_gather(turned, "virt", axis=0, tiled=True),
        half_blocks,
        preferred_element_type=jnp.float32,
    )
    sigma_terms = sigma_terms.reshape(combos * orbitals, row_share)
    return lax.psum_scatter(sigma_terms, "chol", scatter_dimension=0, tiled=True)


def kernel(ring, r_in, l_in, out, rbuf, lbuf, xbuf, xtmp, acc, sendbuf, recvbuf,
           loc_sem, r_send, r_recv, d_send, d_recv, y_send, y_recv, f_send, f_recv,
           p_send, p_recv):
    half = ring // 2
    chol, virt = lax.axis_index("chol"), lax.axis_index("virt")
    core, chip = chol % 2, chol // 2
    odd = chip % 2
    pos = (1 - odd) * (chip // 2) + odd * (ring - 1 - chip // 2)
    vecs, rows, width = l_in.shape
    tall = r_in.shape[0]

    def at(offset):
        there = (pos + offset + ring) % ring
        back = there // half
        q = (1 - back) * 2 * there + back * (2 * (ring - 1 - there) + 1)
        return (q * 2 + core, virt)

    partner, across = (chip * 2 + 1 - core, virt), (chol, 1 - virt)

    barrier = pltpu.get_barrier_semaphore()
    for peer in [at(r) for r in range(1, ring)] + [partner, across]:
        pl.semaphore_signal(barrier, inc=1, device_id=peer, device_id_type=MESH)

    cp_r = pltpu.make_async_copy(r_in, rbuf.at[0, pl.ds(0, tall)], loc_sem.at[0])
    cp_l = pltpu.make_async_copy(l_in, lbuf.at[virt, core], loc_sem.at[1])
    cp_r.start()
    cp_l.start()
    if width > tall:
        rbuf[:, tall:, :] = jnp.zeros((ring, width - tall, width), rbuf.dtype)
    cp_r.wait()
    cp_l.wait()
    pl.semaphore_wait(barrier, ring + 1)

    def remote(src, dst, s, r, to):
        return pltpu.make_async_remote_copy(
            src_ref=src, dst_ref=dst, send_sem=s, recv_sem=r, device_id=to, device_id_type=MESH)

    def hop_up(d):
        return remote(rbuf.at[d - 1, pl.ds(0, tall)], rbuf.at[d, pl.ds(0, tall)],
                      r_send.at[d], r_recv.at[d], at(1))

    def hop_down(d):
        src = 0 if d == ring - 1 else d + 1
        return remote(rbuf.at[src, pl.ds(0, tall)], rbuf.at[d, pl.ds(0, tall)],
                      r_send.at[d], r_recv.at[d], at(-1))

    hops = {d: hop_up(d) for d in range(1, half + 1)}
    hops.update({d: hop_down(d) for d in range(half + 1, ring)})
    give = remote(lbuf.at[virt, core], lbuf.at[virt, core], d_send, d_recv, partner)
    cross = [remote(lbuf.at[virt, core, j], lbuf.at[virt, core, j], y_send.at[j], y_recv.at[j], across)
             for j in range(vecs)]
    share = [remote(lbuf.at[1 - virt, core, j], lbuf.at[1 - virt, core, j], f_send.at[j], f_recv.at[j], partner)
             for j in range(vecs)]

    hops[1].start()
    hops[ring - 1].start()
    for c in cross:
        c.start()
    give.start()

    part = vecs // 2
    chunk = part * rows

    def stage_one(slot, c, j, dst, first):
        left = lbuf[virt, c, pl.ds(j * part, part)].reshape(chunk, width)
        dst[pl.ds(first, chunk), :] = lax.dot_general(
            left, rbuf[slot], (((1,), (1,)), ((), ())),
            preferred_element_type=jnp.float32).astype(jnp.bfloat16)

    def keep(slot, k):
        @pl.loop(0, 4)
        def _(i):
            stage_one(slot, i // 2, i % 2, xbuf.at[k], pl.multiple_of(i * chunk, chunk))

    give.wait_recv()
    keep(0, 0)
    kept = {0: 0}
    moved = 0
    for s in range(1, half + 1):
        due = [s] if s == half else [s, ring - s]
        for d in due:
            hops[d].wait_recv()
        if s < half:
            hops[s + 1].start()
            if ring - s - 1 > half:
                hops[ring - s - 1].start()
        goal = (vecs * s) // half
        for j in range(moved, goal):
            cross[j].wait_recv()
            share[j].start()
        moved = goal
        for d in due:
            if len(kept) < KEPT:
                kept[d] = len(kept)
                keep(d, kept[d])
    for j in range(vecs):
        share[j].wait_recv()

    def second(p, x0, x1):
        both = jnp.concatenate([x0, x1], axis=0)
        c, j = p // vecs, p % vecs
        weights = jnp.concatenate([lbuf[0, c, j], lbuf[1, c, j]], axis=0)
        acc[...] += lax.dot_general(both, weights, (((1,), (1,)), ((), ())),
                                    preferred_element_type=jnp.float32)

    far = sorted((d for d in range(ring) if d not in kept), key=lambda d: -min(d, ring - d))
    near = sorted(kept, key=lambda d: -min(d, ring - d))
    order = far + near
    posts = []
    for g in range(0, ring, 2):
        pair = order[g:g + 2]
        acc[...] = jnp.zeros_like(acc)
        if pair[0] in kept:
            @pl.loop(0, 2 * vecs)
            def _(p):
                first = pl.ds(pl.multiple_of(p * rows, rows), rows)
                second(p, xbuf[kept[pair[0]], first, :], xbuf[kept[pair[1]], first, :])
        else:
            @pl.loop(0, 4)
            def _(i):
                for t in range(2):
                    stage_one(pair[t], i // 2, i % 2, xtmp.at[t], 0)

                @pl.loop(0, part)
                def _(m):
                    first = pl.ds(pl.multiple_of(m * rows, rows), rows)
                    second(i * part + m, xtmp[0, first, :], xtmp[1, first, :])
        for t in range(2):
            d = pair[t]
            if d == 0:
                out[...] = acc[pl.ds(t * rows, rows), :]
            else:
                sendbuf[d - 1] = acc[pl.ds(t * rows, rows), :].astype(jnp.bfloat16)
                post = remote(sendbuf.at[d - 1], recvbuf.at[d - 1], p_send.at[d - 1], p_recv.at[d - 1], at(-d))
                post.start()
                posts.append((d, post))
    for d, post in posts:
        post.wait_recv()
        out[...] += recvbuf[d - 1].astype(jnp.float32)
    for d, post in posts:
        post.wait_send()
    for d in hops:
        hops[d].wait_send()
    for c in cross + share:
        c.wait_send()
    give.wait_send()


def fused(ring, amplitudes, chol_vectors):
    vecs, share, orbitals = chol_vectors.shape
    rows, width, tall = up(share, 16), up(orbitals, 128), up(orbitals, 16)
    bf, f32 = jnp.bfloat16, jnp.float32
    r = jnp.pad(amplitudes, ((0, tall - orbitals), (0, width - orbitals)))
    l = jnp.pad(chol_vectors, ((0, 0), (0, rows - share), (0, width - orbitals)))
    dma = pltpu.SemaphoreType.DMA
    turned = pl.pallas_call(
        functools.partial(kernel, ring),
        out_shape=jax.ShapeDtypeStruct((rows, 2 * rows), f32),
        in_specs=[pl.BlockSpec(memory_space=pl.ANY)] * 2,
        out_specs=pl.BlockSpec(memory_space=pltpu.VMEM),
        scratch_shapes=[
            pltpu.VMEM((ring, width, width), bf),
            pltpu.VMEM((2, 2, vecs, rows, width), bf),
            pltpu.VMEM((KEPT, 2 * vecs * rows, width), bf),
            pltpu.VMEM((2, vecs // 2 * rows, width), bf),
            pltpu.VMEM((2 * rows, 2 * rows), f32),
            pltpu.VMEM((ring - 1, rows, 2 * rows), bf),
            pltpu.VMEM((ring - 1, rows, 2 * rows), bf),
            dma((2,)), dma((ring,)), dma((ring,)), dma, dma,
            dma((vecs,)), dma((vecs,)), dma((vecs,)), dma((vecs,)),
            dma((ring - 1,)), dma((ring - 1,)),
        ],
        compiler_params=pltpu.CompilerParams(
            collective_id=0, has_side_effects=True, vmem_limit_bytes=67043328),
        name="ladder",
    )(r, l)
    sides = jnp.concatenate([turned[:share, :share], turned[:share, rows:rows + share]], axis=1)
    return sides.T


def solution(mesh):
    chol, virt = mesh.shape["chol"], mesh.shape["virt"]

    def shards(amplitudes, chol_vectors):
        vecs, share, orbitals = chol_vectors.shape
        fits = virt == 2 and chol % 4 == 0 and chol >= 16 and vecs % 2 == 0
        if fits and amplitudes.shape[0] == orbitals:
            return fused(chol // 2, amplitudes, chol_vectors)
        return plain(amplitudes, chol_vectors)

    placed = (P("chol", None), P("chol", "virt", None))
    return jax.shard_map(
        shards, mesh=mesh, in_specs=placed, out_specs=P("chol", "virt"), check_vma=False
    )
```
